32 devices in a mesh: seq: 8 (over z, y), head: 4 (over x, core).
Axes of the slice: x: 2, y: 2, z: 4, core: 2. Of those that a mesh axis runs over, the one named last changes fastest.
Arguments:
- queries: bfloat16 [2048, 4096], P(('seq', 'head')), may hold values from -9 to 9, as said below
- keys: bfloat16 [2048, 512], P(('seq', 'head')), may hold values from -9 to 9, as said below
- values: bfloat16 [2048, 512], P(('seq', 'head')), may hold values from -6 to 6
Outputs:
- attended: bfloat16 [2048, 4096], P(('seq', 'head'))
The draws below stay inside these ranges and needn't reach their ends.
Inputs may be any that keep to these rules, and one draw needn't show every extreme that they name: `queries`: query entries are of order one except on a few rows. `keys`: key entries are of order one except on a few rows.
All inputs are finite; a program needn't handle non-finite values.
Results may differ from the reference program's by a relative error of at most 0.005.
Values may be sent and summed in bfloat16 or wider, within the bound.
A program may use at most 64 MiB of HBM per device.

```python
import math
import jax
import jax.numpy as jnp
from jax import lax

H = 32
KV = 4
DH = 128
TOKENS = 2048


def paired(key):
    base = jax.random.fold_in(key, 7)
    key_q, key_k = jax.random.split(base, 2)
    query_mat = jnp.clip(jax.random.normal(key_q, (TOKENS, H * DH), jnp.float32), -6.0, 6.0)
    key_mat = jnp.clip(jax.random.normal(key_k, (TOKENS, KV * DH), jnp.float32), -6.0, 6.0)
    return (query_mat, key_mat)


def draw_queries(key, part):
    return paired(key)[0].astype(jnp.bfloat16)


def draw_keys(key, part):
    return paired(key)[1].astype(jnp.bfloat16)


def shard_levels(key, dims, pieces, smallest, high):
    factor_of, own = 1.0, jax.random.fold_in(key, 6)
    for position, shards_of in pieces:
        draws = jnp.exp(jax.random.uniform(jax.random.fold_in(own, position), (shards_of,), jnp.float32, smallest / len(pieces), high / len(pieces)))
        factor_of = factor_of * jnp.repeat(draws, dims[position] // shards_of).reshape([-1 if axis == position else 1 for axis in range(len(dims))])
    return factor_of


def scatter_about(rng, dims, spread, bound, shards=(), kind=jnp.bfloat16):
    array = spread * jax.random.normal(rng, dims, jnp.float32)
    if shards:
        array = array * shard_levels(rng, dims, shards, -0.22, 0.18)
    return jnp.clip(array, -bound, bound).astype(kind)


def setup_inputs(seed: int = 0) -> dict:
    seeds = jax.random.split(jax.random.key(seed), 4)
    queries = draw_queries(jax.random.fold_in(seeds[3], 71), 0)
    keys = draw_keys(jax.random.fold_in(seeds[3], 71), 0)
    values = scatter_about(seeds[2], (TOKENS, KV * DH), 1.0, 6.0, ((0, 32),))
    return dict(queries=queries, keys=keys, values=values)


def reference(queries, keys, values):
    length = queries.shape[0]
    block = min(1024, length)
    blocks = length // block
    group = H // KV
    scale = 1.0 / math.sqrt(DH)
    q_heads = queries.reshape(length, H, DH)
    k_heads = keys.reshape(length, KV, DH)
    v_heads = values.reshape(length, KV, DH)
    key_pos = jnp.arange(length, dtype=jnp.int32)

    def one_head(head):
        q_mat = lax.dynamic_index_in_dim(q_heads, head, 1, keepdims=False)
        k_mat = lax.dynamic_index_in_dim(k_heads, head // group, 1, keepdims=False)
        v_mat = lax.dynamic_index_in_dim(v_heads, head // group, 1, keepdims=False)

        def one_block(index):
            first = (index * block).astype(jnp.int32)
            rows = lax.dynamic_slice_in_dim(q_mat, first, block, 0)
            scores = jnp.dot(rows, k_mat.T, preferred_element_type=jnp.float32) * scale
            query_pos = first + jnp.arange(block, dtype=jnp.int32)
            scores = jnp.where(key_pos[None, :] <= query_pos[:, None], scores, -jnp.inf)
            rowmax = lax.optimization_barrier(jnp.max(scores, axis=1, keepdims=True))
            expo = jnp.exp(scores - rowmax)
            total = lax.optimization_barrier(jnp.sum(expo, axis=1, keepdims=True))
            numer = jnp.dot(expo.astype(jnp.bfloat16), v_mat, preferred_element_type=jnp.float32)
            return (numer / total).astype(jnp.bfloat16)
        return lax.map(one_block, jnp.arange(blocks, dtype=jnp.int32)).reshape(length, DH)
    result = lax.map(one_head, jnp.arange(H, dtype=jnp.int32))
    return result.transpose(1, 0, 2).reshape(length, H * DH)
```

```python
import functools
import math

import jax
import jax.numpy as jnp
from jax import lax
from jax.experimental import pallas as pl
from jax.experimental.pallas import tpu as pltpu
from jax.sharding import PartitionSpec as P

H = 32
KV = 4
DH = 128
GROUP = H // KV
PLANE = 8
Z, X, Y, DK, DV, C0 = 0, 1, 2, 3, 4, 5
KINDS = C0 + 4


def kernel(n_head, planes, q_hbm, k_hbm, v_hbm, o_ref, kv, q, mx, acc, lsem, send, recv):
    tok = k_hbm.shape[0]
    me = lax.axis_index("seq") * n_head + lax.axis_index("head")
    core = lax.rem(me, 2)
    x = lax.rem(lax.div(me, 2), 2)
    y = lax.rem(lax.div(me, 4), 2)
    z = lax.div(me, PLANE)

    def dev(linear):
        return (lax.div(linear, n_head), lax.rem(linear, n_head))

    to_x = dev(me + 2 - 4 * x)
    to_y = dev(me + 4 - 8 * y)
    to_core = dev(me + 1 - 2 * core)
    up = dev(lax.min(me + PLANE, planes * PLANE - 1))
    down = dev(lax.max(me - PLANE, 0))

    own_k = pltpu.make_async_copy(k_hbm, kv.at[me, 0], lsem.at[0])
    own_v = pltpu.make_async_copy(v_hbm, kv.at[me, 1], lsem.at[1])
    own_q = pltpu.make_async_copy(q_hbm, q, lsem.at[2])
    own_k.start()
    own_v.start()
    own_q.start()

    barrier = pltpu.get_barrier_semaphore()

    def greet(where):
        pl.semaphore_signal(barrier, inc=1, device_id=where, device_id_type=pl.DeviceIdType.MESH)

    greet(to_x)
    greet(to_y)
    greet(to_core)

    @pl.when(z < planes - 1)
    def _():
        greet(up)

    @pl.when(z > 0)
    def _():
        greet(down)

    pl.semaphore_wait(barrier, 3 + lax.min(z, 1) + lax.min(planes - 1 - z, 1))

    own_k.wait()
    own_v.wait()

    def slot(k, yy, xx, cc):
        return (z - k) * PLANE + yy * 4 + xx * 2 + cc

    def copy(kind, k, where, block, half=None, later=0):
        ref = kv.at[block] if half is None else kv.at[block, half]
        return pltpu.make_async_remote_copy(
            src_ref=ref,
            dst_ref=ref,
            send_sem=send.at[kind, k],
            recv_sem=recv.at[kind, k + later],
            device_id=where,
            device_id_type=pl.DeviceIdType.MESH,
        )

    def out_z(k):
        return copy(Z, k, up, slot(k, y, x, core), later=1)

    def outs(k):
        mine, xs, ys, diag = (
            slot(k, y, x, core),
            slot(k, y, 1 - x, core),
            slot(k, 1 - y, x, core),
            slot(k, 1 - y, 1 - x, core),
        )
        return dict(
            x=lambda: copy(X, k, to_x, mine),
            y=lambda: copy(Y, k, to_y, mine),
            c0=lambda: copy(C0, k, to_core, mine),
            dk=lambda: copy(DK, k, to_y, xs, 0),
            c1=lambda: copy(C0 + 1, k, to_core, xs),
            dv=lambda: copy(DV, k, to_x, ys, 1),
            c2=lambda: copy(C0 + 2, k, to_core, ys),
            c3=lambda: copy(C0 + 3, k, to_core, diag),
        )

    def ins(k):
        def landed(kind, block, half=None):
            copy(kind, k, to_x, block, half).wait_recv()

        other = 1 - core
        return dict(
            z=lambda: landed(Z, slot(k, y, x, core)),
            x=lambda: landed(X, slot(k, y, 1 - x, core)),
            y=lambda: landed(Y, slot(k, 1 - y, x, core)),
            dk=lambda: landed(DK, slot(k, 1 - y, 1 - x, core), 0),
            dv=lambda: landed(DV, slot(k, 1 - y, 1 - x, core), 1),
            c0=lambda: landed(C0, slot(k, y, x, other)),
            c1=lambda: landed(C0 + 1, slot(k, y, 1 - x, other)),
            c2=lambda: landed(C0 + 2, slot(k, 1 - y, x, other)),
            c3=lambda: landed(C0 + 3, slot(k, 1 - y, 1 - x, other)),
        )

    def launch(k):
        o = outs(k)

        @pl.when(z < planes - 1)
        def _():
            out_z(k).start()

        o["x"]().start()
        o["y"]().start()
        o["c0"]().start()

    scale = math.log2(math.e) / math.sqrt(DH)
    width = PLANE * tok
    rows = GROUP * tok

    def chunk(k, first):
        base = (z - k) * PLANE
        for g in range(KV):
            cols = slice(g * DH, (g + 1) * DH)
            kk = kv[pl.ds(base, PLANE), 0, :, cols].reshape(width, DH)
            vv = kv[pl.ds(base, PLANE), 1, :, cols].reshape(width, DH)
            vv = jnp.concatenate([vv, jnp.ones_like(vv)], axis=1)
            qq = jnp.concatenate(
                [q[:, (g * GROUP + h) * DH : (g * GROUP + h + 1) * DH] for h in range(GROUP)], axis=0
            )
            s = lax.dot_general(
                qq, kk, (((1,), (1,)), ((), ())), preferred_element_type=jnp.float32
            )
            if first:
                row = lax.rem(lax.broadcasted_iota(jnp.int32, (rows, width), 0), tok)
                col = lax.broadcasted_iota(jnp.int32, (rows, width), 1)
                s = jnp.where(col <= row + lax.rem(me, PLANE) * tok, s, -jnp.inf)
            top = jnp.max(s, axis=1, keepdims=True)
            if not first:
                old = mx[g, :, :1]
                top = jnp.maximum(old, top)
            p = jnp.exp2((s - top) * scale).astype(jnp.bfloat16)
            pv = jnp.dot(p, vv, preferred_element_type=jnp.float32)
            if not first:
                pv += acc[g] * jnp.exp2((old - top) * scale)
            acc[g] = pv
            mx[g] = jnp.broadcast_to(top, (rows, DH))

    def step(k, first):
        i, o = ins(k), outs(k)
        i["x"]()
        o["dk"]().start()
        o["c1"]().start()
        i["y"]()
        o["dv"]().start()
        o["c2"]().start()

        @pl.when(k < z)
        def _():
            ins(k + 1)["z"]()
            launch(k + 1)

        i["dk"]()
        i["dv"]()
        o["c3"]().start()
        for name in ("c0", "c1", "c2", "c3"):
            i[name]()
        chunk(k, first)

    launch(0)
    own_q.wait()
    step(0, True)

    def body(k, carry):
        step(k, False)
        return carry

    lax.fori_loop(1, z + 1, body, 0)

    for g in range(KV):
        out = (acc[g, :, :DH] / acc[g, :, DH:]).astype(o_ref.dtype)
        for h in range(GROUP):
            o_ref[:, (g * GROUP + h) * DH : (g * GROUP + h + 1) * DH] = out[h * tok : (h + 1) * tok]

    def drain(k, carry):
        @pl.when(z < planes - 1)
        def _():
            out_z(k).wait_send()

        for c in outs(k).values():
            c().wait_send()
        return carry

    lax.fori_loop(0, z + 1, drain, 0)


def per_device(queries, keys, values):
    n_head = lax.axis_size("head")
    devices = n_head * lax.axis_size("seq")
    planes = devices // PLANE
    tok = queries.shape[0]
    rows = GROUP * tok
    hbm = pl.BlockSpec(memory_space=pl.ANY)
    return pl.pallas_call(
        functools.partial(kernel, n_head, planes),
        out_shape=jax.ShapeDtypeStruct(queries.shape, queries.dtype),
        in_specs=[hbm] * 3,
        out_specs=pl.BlockSpec(memory_space=pltpu.VMEM),
        scratch_shapes=[
            pltpu.VMEM((devices, 2, tok, KV * DH), jnp.bfloat16),
            pltpu.VMEM(queries.shape, jnp.bfloat16),
            pltpu.VMEM((KV, rows, DH), jnp.float32),
            pltpu.VMEM((KV, rows, 2 * DH), jnp.float32),
            pltpu.SemaphoreType.DMA((3,)),
            pltpu.SemaphoreType.DMA((KINDS, planes)),
            pltpu.SemaphoreType.DMA((KINDS, planes)),
        ],
        compiler_params=pltpu.CompilerParams(
            collective_id=0, has_side_effects=True, vmem_limit_bytes=60 * 1024 * 1024
        ),
        name="relay_attention",
    )(queries, keys, values)


def solution(mesh):
    spec = P(("seq", "head"), None)
    return jax.shard_map(
        per_device, mesh=mesh, in_specs=(spec, spec, spec), out_specs=spec, check_vma=False
    )
```

```python
import functools
import math

import jax
import jax.numpy as jnp
from jax import lax
from jax.experimental import pallas as pl
from jax.experimental.pallas import tpu as pltpu
from jax.sharding import PartitionSpec as P

H = 32
KV = 4
DH = 128
GROUP = H // KV
PLANE = 8
Z, X, Y, DK, DV, C0 = 0, 2, 4, 6, 7, 8
KINDS = C0 + 4


def kernel(n_head, planes, q_hbm, k_hbm, v_hbm, o_ref, kv, q, mx, acc, lsem, send, recv):
    tok = k_hbm.shape[0]
    me = lax.axis_index("seq") * n_head + lax.axis_index("head")
    core = lax.rem(me, 2)
    x = lax.rem(lax.div(me, 2), 2)
    y = lax.rem(lax.div(me, 4), 2)
    z = lax.div(me, PLANE)

    def dev(linear):
        return (lax.div(linear, n_head), lax.rem(linear, n_head))

    to_x = dev(me + 2 - 4 * x)
    to_y = dev(me + 4 - 8 * y)
    to_core = dev(me + 1 - 2 * core)
    up = dev(lax.min(me + PLANE, planes * PLANE - 1))
    down = dev(lax.max(me - PLANE, 0))

    own_k = pltpu.make_async_copy(k_hbm, kv.at[me, 0], lsem.at[0])
    own_v = pltpu.make_async_copy(v_hbm, kv.at[me, 1], lsem.at[1])
    own_q = pltpu.make_async_copy(q_hbm, q, lsem.at[2])
    own_k.start()
    own_v.start()
    own_q.start()

    barrier = pltpu.get_barrier_semaphore()

    def greet(where):
        pl.semaphore_signal(barrier, inc=1, device_id=where, device_id_type=pl.DeviceIdType.MESH)

    greet(to_x)
    greet(to_y)
    greet(to_core)

    @pl.when(z < planes - 1)
    def _():
        greet(up)

    @pl.when(z > 0)
    def _():
        greet(down)

    pl.semaphore_wait(barrier, 3 + lax.min(z, 1) + lax.min(planes - 1 - z, 1))

    own_k.wait()
    own_v.wait()

    def slot(k, yy, xx, cc):
        return (z - k) * PLANE + yy * 4 + xx * 2 + cc

    def copy(kind, k, where, block, half=None, later=0):
        ref = kv.at[block] if half is None else kv.at[block, half]
        return pltpu.make_async_remote_copy(
            src_ref=ref,
            dst_ref=ref,
            send_sem=send.at[kind, k],
            recv_sem=recv.at[kind, k + later],
            device_id=where,
            device_id_type=pl.DeviceIdType.MESH,
        )

    def out_z(k, half):
        return copy(Z + half, k, up, slot(k, y, x, core), half, later=1)

    def outs(k):
        mine, xs, ys, diag = (
            slot(k, y, x, core),
            slot(k, y, 1 - x, core),
            slot(k, 1 - y, x, core),
            slot(k, 1 - y, 1 - x, core),
        )
        return dict(
            xk=lambda: copy(X, k, to_x, mine, 0),
            xv=lambda: copy(X + 1, k, to_x, mine, 1),
            yk=lambda: copy(Y, k, to_y, mine, 0),
            yv=lambda: copy(Y + 1, k, to_y, mine, 1),
            dk=lambda: copy(DK, k, to_y, xs, 0),
            dv=lambda: copy(DV, k, to_x, ys, 1),
            c0=lambda: copy(C0, k, to_core, mine),
            c1=lambda: copy(C0 + 1, k, to_core, xs),
            c2=lambda: copy(C0 + 2, k, to_core, ys),
            c3=lambda: copy(C0 + 3, k, to_core, diag),
        )

    def landed(kind, k, block, half=None):
        copy(kind, k, to_x, block, half).wait_recv()

    def send_up(k, half):
        @pl.when(z < planes - 1)
        def _():
            out_z(k, half).start()

    scale = math.log2(math.e) / math.sqrt(DH)
    rows = GROUP * tok

    def chunk(k, first, heads=range(KV), side=None):
        blocks = PLANE if side is None else PLANE // 2
        base = (z - k) * PLANE + (0 if side is None else side * blocks)
        width = blocks * tok
        for g in heads:
            cols = slice(g * DH, (g + 1) * DH)
            kk = kv[pl.ds(base, blocks), 0, :, cols].reshape(width, DH)
            vv = kv[pl.ds(base, blocks), 1, :, cols].reshape(width, DH)
            vv = jnp.concatenate([vv, jnp.ones_like(vv)], axis=1)
            qq = jnp.concatenate(
                [q[:, (g * GROUP + h) * DH : (g * GROUP + h + 1) * DH] for h in range(GROUP)], axis=0
            )
            s = lax.dot_general(
                qq, kk, (((1,), (1,)), ((), ())), preferred_element_type=jnp.float32
            )
            if first:
                row = lax.rem(lax.broadcasted_iota(jnp.int32, (rows, width), 0), tok)
                col = lax.broadcasted_iota(jnp.int32, (rows, width), 1)
                s = jnp.where(col <= row + lax.rem(me, PLANE) * tok, s, -jnp.inf)
            top = jnp.max(s, axis=1, keepdims=True)
            if not first:
                old = mx[g, :, :1]
                top = jnp.maximum(old, top)
            p = jnp.exp2((s - top) * scale).astype(jnp.bfloat16)
            pv = jnp.dot(p, vv, preferred_element_type=jnp.float32)
            if not first:
                pv += acc[g] * jnp.exp2((old - top) * scale)
            acc[g] = pv
            mx[g] = jnp.broadcast_to(top, (rows, DH))

    def relay_first(k):
        o = outs(k)

        @pl.when(k < z)
        def _():
            landed(Z, k + 1, slot(k + 1, y, x, core), 0)
            send_up(k + 1, 0)
            outs(k + 1)["xk"]().start()

        landed(X, k, slot(k, y, 1 - x, core), 0)
        o["dk"]().start()
        landed(Y + 1, k, slot(k, 1 - y, x, core), 1)
        o["dv"]().start()

    def relay_mid(k):
        o = outs(k)

        @pl.when(k < z)
        def _():
            landed(Z + 1, k + 1, slot(k + 1, y, x, core), 1)
            send_up(k + 1, 1)
            later = outs(k + 1)
            later["yv"]().start()
            later["xv"]().start()
            later["yk"]().start()
            later["c0"]().start()

        landed(X + 1, k, slot(k, y, 1 - x, core), 1)
        o["c1"]().start()
        landed(Y, k, slot(k, 1 - y, x, core), 0)
        o["c2"]().start()

    def relay_second(k):
        diag = slot(k, 1 - y, 1 - x, core)
        landed(DK, k, diag, 0)
        landed(DV, k, diag, 1)
        outs(k)["c3"]().start()

    def relay_near(k):
        landed(C0, k, slot(k, y, x, 1 - core))
        landed(C0 + 1, k, slot(k, y, 1 - x, 1 - core))

    def relay_far(k):
        landed(C0 + 2, k, slot(k, 1 - y, x, 1 - core))
        landed(C0 + 3, k, slot(k, 1 - y, 1 - x, 1 - core))

    o = outs(0)
    for half in (0, 1):
        send_up(0, half)
    for name in ("xk", "yv", "xv", "yk", "c0"):
        o[name]().start()
    own_q.wait()
    relay_first(0)
    relay_mid(0)
    relay_second(0)
    relay_near(0)
    relay_far(0)

    @pl.when(z > 0)
    def _():
        relay_first(1)
        chunk(0, True, (0, 1))
        relay_mid(1)
        chunk(0, True, (2, 3))
        relay_second(1)

    @pl.when(z == 0)
    def _():
        chunk(0, True)

    def body(k, carry):
        relay_near(k - 1)
        relay_far(k - 1)
        relay_first(k)
        chunk(k - 1, False, (0, 1))
        relay_mid(k)
        chunk(k - 1, False, (2, 3))
        relay_second(k)
        return carry

    lax.fori_loop(2, z + 1, body, 0)

    @pl.when(z > 0)
    def _():
        relay_near(z)
        chunk(z, False, side=y)
        relay_far(z)
        chunk(z, False, side=1 - y)

    for g in range(KV):
        out = (acc[g, :, :DH] / acc[g, :, DH:]).astype(o_ref.dtype)
        for h in range(GROUP):
            o_ref[:, (g * GROUP + h) * DH : (g * GROUP + h + 1) * DH] = out[h * tok : (h + 1) * tok]

    def drain(k, carry):
        @pl.when(z < planes - 1)
        def _():
            for half in (0, 1):
                out_z(k, half).wait_send()

        for c in outs(k).values():
            c().wait_send()
        return carry

    lax.fori_loop(0, z + 1, drain, 0)


def per_device(queries, keys, values):
    n_head = lax.axis_size("head")
    devices = n_head * lax.axis_size("seq")
    planes = devices // PLANE
    tok = queries.shape[0]
    rows = GROUP * tok
    hbm = pl.BlockSpec(memory_space=pl.ANY)
    return pl.pallas_call(
        functools.partial(kernel, n_head, planes),
        out_shape=pltpu.VMEM(queries.shape, queries.dtype),
        in_specs=[hbm] * 3,
        out_specs=pl.BlockSpec(memory_space=pltpu.VMEM),
        scratch_shapes=[
            pltpu.VMEM((devices, 2, tok, KV * DH), jnp.bfloat16),
            pltpu.VMEM(queries.shape, jnp.bfloat16),
            pltpu.VMEM((KV, rows, DH), jnp.float32),
            pltpu.VMEM((KV, rows, 2 * DH), jnp.float32),
            pltpu.SemaphoreType.DMA((3,)),
            pltpu.SemaphoreType.DMA((KINDS, planes)),
            pltpu.SemaphoreType.DMA((KINDS, planes)),
        ],
        compiler_params=pltpu.CompilerParams(
            collective_id=0, has_side_effects=True, vmem_limit_bytes=60 * 1024 * 1024
        ),
        name="relay_attention",
    )(queries, keys, values)


def solution(mesh):
    spec = P(("seq", "head"), None)
    return jax.shard_map(
        per_device, mesh=mesh, in_specs=(spec, spec, spec), out_specs=spec, check_vma=False
    )
```

```python
import functools
import math

import jax
import jax.numpy as jnp
from jax import lax
from jax.experimental import pallas as pl
from jax.experimental.pallas import tpu as pltpu
from jax.sharding import PartitionSpec as P

H = 32
KV = 4
DH = 128
GROUP = H // KV
PLANE = 8
Z, X, Y, DK, DV, C0 = 0, 2, 4, 6, 7, 8
KINDS = C0 + 4


def kernel(n_head, planes, q_hbm, k_hbm, v_hbm, o_ref, kv, q, mx, tot, acc, lsem, send, recv):
    tok = k_hbm.shape[0]
    me = lax.axis_index("seq") * n_head + lax.axis_index("head")
    core = lax.rem(me, 2)
    x = lax.rem(lax.div(me, 2), 2)
    y = lax.rem(lax.div(me, 4), 2)
    z = lax.div(me, PLANE)

    def dev(linear):
        return (lax.div(linear, n_head), lax.rem(linear, n_head))

    to_x = dev(me + 2 - 4 * x)
    to_y = dev(me + 4 - 8 * y)
    to_core = dev(me + 1 - 2 * core)
    up = dev(lax.min(me + PLANE, planes * PLANE - 1))
    down = dev(lax.max(me - PLANE, 0))

    own_k = pltpu.make_async_copy(k_hbm, kv.at[me, 0], lsem.at[0])
    own_v = pltpu.make_async_copy(v_hbm, kv.at[me, 1], lsem.at[1])
    own_q = pltpu.make_async_copy(q_hbm, q, lsem.at[2])
    own_k.start()
    own_v.start()
    own_q.start()

    barrier = pltpu.get_barrier_semaphore()

    def greet(where):
        pl.semaphore_signal(barrier, inc=1, device_id=where, device_id_type=pl.DeviceIdType.MESH)

    greet(to_x)
    greet(to_y)
    greet(to_core)

    @pl.when(z < planes - 1)
    def _():
        greet(up)

    @pl.when(z > 0)
    def _():
        greet(down)

    pl.semaphore_wait(barrier, 3 + lax.min(z, 1) + lax.min(planes - 1 - z, 1))

    own_k.wait()
    own_v.wait()

    def slot(k, yy, xx, cc):
        return (z - k) * PLANE + yy * 4 + xx * 2 + cc

    def copy(kind, k, where, block, half=None, later=0):
        ref = kv.at[block] if half is None else kv.at[block, half]
        return pltpu.make_async_remote_copy(
            src_ref=ref,
            dst_ref=ref,
            send_sem=send.at[kind, k],
            recv_sem=recv.at[kind, k + later],
            device_id=where,
            device_id_type=pl.DeviceIdType.MESH,
        )

    def out_z(k, half):
        return copy(Z + half, k, up, slot(k, y, x, core), half, later=1)

    def outs(k):
        mine, xs, ys, diag = (
            slot(k, y, x, core),
            slot(k, y, 1 - x, core),
            slot(k, 1 - y, x, core),
            slot(k, 1 - y, 1 - x, core),
        )
        return dict(
            xk=lambda: copy(X, k, to_x, mine, 0),
            xv=lambda: copy(X + 1, k, to_x, mine, 1),
            yk=lambda: copy(Y, k, to_y, mine, 0),
            yv=lambda: copy(Y + 1, k, to_y, mine, 1),
            dk=lambda: copy(DK, k, to_y, xs, 0),
            dv=lambda: copy(DV, k, to_x, ys, 1),
            c0=lambda: copy(C0, k, to_core, mine),
            c1=lambda: copy(C0 + 1, k, to_core, xs),
            c2=lambda: copy(C0 + 2, k, to_core, ys),
            c3=lambda: copy(C0 + 3, k, to_core, diag),
        )

    def landed(kind, k, block, half=None):
        copy(kind, k, to_x, block, half).wait_recv()

    def send_up(k, half):
        @pl.when(z < planes - 1)
        def _():
            out_z(k, half).start()

    scale = math.log2(math.e) / math.sqrt(DH)
    rows = GROUP * tok

    def chunk(k, first, heads=range(KV), side=None):
        blocks = PLANE if side is None else PLANE // 2
        base = (z - k) * PLANE + (0 if side is None else side * blocks)
        width = blocks * tok
        for g in heads:
            cols = slice(g * DH, (g + 1) * DH)
            kk = kv[pl.ds(base, blocks), 0, :, cols].reshape(width, DH)
            vv = kv[pl.ds(base, blocks), 1, :, cols].reshape(width, DH)
            qq = jnp.concatenate(
                [q[:, (g * GROUP + h) * DH : (g * GROUP + h + 1) * DH] for h in range(GROUP)], axis=0
            )
            s = lax.dot_general(
                kk, qq, (((1,), (1,)), ((), ())), preferred_element_type=jnp.float32
            )
            if first:
                key = lax.broadcasted_iota(jnp.int32, (width, rows), 0)
                row = lax.rem(lax.broadcasted_iota(jnp.int32, (width, rows), 1), tok)
                s = jnp.where(key <= row + lax.rem(me, PLANE) * tok, s, -jnp.inf)
            top = jnp.max(s, axis=0, keepdims=True)
            if not first:
                old = mx[g]
                top = jnp.maximum(old, top)
            p = jnp.exp2((s - top) * scale)
            total = jnp.sum(p, axis=0, keepdims=True)
            pv = lax.dot_general(
                vv,
                p.astype(jnp.bfloat16),
                (((0,), (0,)), ((), ())),
                preferred_element_type=jnp.float32,
            )
            if not first:
                factor = jnp.exp2((old - top) * scale)
                total += tot[g] * factor
                pv += acc[g] * factor
            acc[g] = pv
            tot[g] = total
            mx[g] = top

    def relay_first(k):
        o = outs(k)

        @pl.when(k < z)
        def _():
            landed(Z, k + 1, slot(k + 1, y, x, core), 0)
            send_up(k + 1, 0)
            outs(k + 1)["xk"]().start()

        landed(X, k, slot(k, y, 1 - x, core), 0)
        o["dk"]().start()
        landed(Y + 1, k, slot(k, 1 - y, x, core), 1)
        o["dv"]().start()

    def relay_mid(k):
        o = outs(k)

        @pl.when(k < z)
        def _():
            landed(Z + 1, k + 1, slot(k + 1, y, x, core), 1)
            send_up(k + 1, 1)
            later = outs(k + 1)
            later["yv"]().start()
            later["xv"]().start()
            later["yk"]().start()
            later["c0"]().start()

        landed(X + 1, k, slot(k, y, 1 - x, core), 1)
        o["c1"]().start()
        landed(Y, k, slot(k, 1 - y, x, core), 0)
        o["c2"]().start()

    def relay_second(k):
        diag = slot(k, 1 - y, 1 - x, core)
        landed(DK, k, diag, 0)
        landed(DV, k, diag, 1)
        outs(k)["c3"]().start()

    def relay_near(k):
        landed(C0, k, slot(k, y, x, 1 - core))
        landed(C0 + 1, k, slot(k, y, 1 - x, 1 - core))

    def relay_far(k):
        landed(C0 + 2, k, slot(k, 1 - y, x, 1 - core))
        landed(C0 + 3, k, slot(k, 1 - y, 1 - x, 1 - core))

    o = outs(0)
    for half in (0, 1):
        send_up(0, half)
    for name in ("xk", "yv", "xv", "yk", "c0"):
        o[name]().start()
    own_q.wait()
    relay_first(0)
    relay_mid(0)
    relay_second(0)
    relay_near(0)
    relay_far(0)

    @pl.when(z > 0)
    def _():
        relay_first(1)
        chunk(0, True, (0, 1))
        relay_mid(1)
        chunk(0, True, (2, 3))
        relay_second(1)

    @pl.when(z == 0)
    def _():
        chunk(0, True)

    def body(k, carry):
        relay_near(k - 1)
        relay_far(k - 1)
        relay_first(k)
        chunk(k - 1, False, (0, 1))
        relay_mid(k)
        chunk(k - 1, False, (2, 3))
        relay_second(k)
        return carry

    lax.fori_loop(2, z + 1, body, 0)

    @pl.when(z > 0)
    def _():
        relay_near(z)
        chunk(z, False, side=y)
        relay_far(z)
        chunk(z, False, side=1 - y)

    for g in range(KV):
        out = (acc[g] / tot[g]).T.astype(o_ref.dtype)
        for h in range(GROUP):
            o_ref[:, (g * GROUP + h) * DH : (g * GROUP + h + 1) * DH] = out[h * tok : (h + 1) * tok]

    def drain(k, carry):
        @pl.when(z < planes - 1)
        def _():
            for half in (0, 1):
                out_z(k, half).wait_send()

        for c in outs(k).values():
            c().wait_send()
        return carry

    lax.fori_loop(0, z + 1, drain, 0)


def per_device(queries, keys, values):
    n_head = lax.axis_size("head")
    devices = n_head * lax.axis_size("seq")
    planes = devices // PLANE
    tok = queries.shape[0]
    rows = GROUP * tok
    hbm = pl.BlockSpec(memory_space=pl.ANY)
    return pl.pallas_call(
        functools.partial(kernel, n_head, planes),
        out_shape=pltpu.VMEM(queries.shape, queries.dtype),
        in_specs=[hbm] * 3,
        out_specs=pl.BlockSpec(memory_space=pltpu.VMEM),
        scratch_shapes=[
            pltpu.VMEM((devices, 2, tok, KV * DH), jnp.bfloat16),
            pltpu.VMEM(queries.shape, jnp.bfloat16),
            pltpu.VMEM((KV, 1, rows), jnp.float32),
            pltpu.VMEM((KV, 1, rows), jnp.float32),
            pltpu.VMEM((KV, DH, rows), jnp.float32),
            pltpu.SemaphoreType.DMA((3,)),
            pltpu.SemaphoreType.DMA((KINDS, planes)),
            pltpu.SemaphoreType.DMA((KINDS, planes)),
        ],
        compiler_params=pltpu.CompilerParams(
            collective_id=0, has_side_effects=True, vmem_limit_bytes=60 * 1024 * 1024
        ),
        name="relay_attention",
    )(queries, keys, values)


def solution(mesh):
    spec = P(("seq", "head"), None)
    return jax.shard_map(
        per_device, mesh=mesh, in_specs=(spec, spec, spec), out_specs=spec, check_vma=False
    )
```
